32 devices in a mesh: rep: 1, dp: 32 (over x, y, z, core).
Axes of the slice: x: 2, y: 2, z: 4, core: 2. Of those that a mesh axis runs over, the one named last changes fastest.
Arguments:
- g_w_gate: bfloat16 [32, 2, 1024, 5120], P(('rep', 'dp'))
- g_w_up: bfloat16 [32, 2, 1024, 5120], P(('rep', 'dp'))
- g_w_down: bfloat16 [32, 2, 5120, 1024], P(('rep', 'dp'))
- w_gate: bfloat16 [2, 1024, 5120], replicated
- w_up: bfloat16 [2, 1024, 5120], replicated
- w_down: bfloat16 [2, 5120, 1024], replicated
- m_w_gate: float32 [2, 1024, 5120], P(None, 'dp')
- m_w_up: float32 [2, 1024, 5120], P(None, 'dp')
- m_w_down: float32 [2, 5120, 1024], P(None, 'dp')
- v_w_gate: float32 [2, 1024, 5120], P(None, 'dp')
- v_w_up: float32 [2, 1024, 5120], P(None, 'dp')
- v_w_down: float32 [2, 5120, 1024], P(None, 'dp')
Outputs:
- output 1: bfloat16 [2, 1024, 5120], P('rep')
- output 2: bfloat16 [2, 1024, 5120], P('rep')
- output 3: bfloat16 [2, 5120, 1024], P('rep')
- output 4: float32 [2, 1024, 5120], P('rep', 'dp')
- output 5: float32 [2, 1024, 5120], P('rep', 'dp')
- output 6: float32 [2, 5120, 1024], P('rep', 'dp')
- output 7: float32 [2, 1024, 5120], P('rep', 'dp')
- output 8: float32 [2, 1024, 5120], P('rep', 'dp')
- output 9: float32 [2, 5120, 1024], P('rep', 'dp')
All inputs are finite; a program needn't handle non-finite values.
Results may differ from the reference program's by a relative error of at most 0.022.
Values are sent between devices in bfloat16 or wider.
A program may use at most 2 GiB of HBM per device.

```python
import jax
import jax.numpy as jnp
from jax import lax

DEVICES = 32
D = 1024
FF = 5120
LAYERS = 2
NAMES = ("w_gate", "w_up", "w_down")
SHAPES = {"w_gate": (LAYERS, D, FF), "w_up": (LAYERS, D, FF), "w_down": (LAYERS, FF, D)}


def setup_inputs(seed: int = 0, part: int = 0) -> dict:
    kz, *keys = jax.random.split(jax.random.key(seed), 1 + 5 * len(NAMES))
    loud = 2.0 ** jax.random.uniform(kz, (), jnp.float32, -1.0, 1.0)
    drawn = {}
    for name, key, both in zip(NAMES, keys[:3], keys[3:6], strict=True):
        own = jax.random.normal(jax.random.fold_in(key, part), (DEVICES, *SHAPES[name]), jnp.float32)
        shared = jax.random.normal(jax.random.fold_in(both, part), SHAPES[name], jnp.float32)
        drawn["g_" + name] = (loud * (0.7 * shared / DEVICES + 0.7 * own * DEVICES**-0.5)).astype(jnp.bfloat16)
    for name, key in zip(NAMES, keys[6:9], strict=True):
        drawn[name] = (jax.random.normal(key, SHAPES[name], jnp.float32) * SHAPES[name][1] ** -0.5).astype(jnp.bfloat16)
    for name, key in zip(NAMES, keys[9:12], strict=True):
        drawn["m_" + name] = loud * 0.5 * jax.random.normal(key, SHAPES[name], jnp.float32)
    for name, key in zip(NAMES, keys[12:15], strict=True):
        drawn["v_" + name] = loud * loud * jax.random.uniform(key, SHAPES[name], jnp.float32, 0.5, 1.5)
    return drawn


def adamw(w, m, v, g):
    m = 0.9 * m + 0.1 * g
    v = 0.95 * v + 0.05 * g * g
    step = m * lax.rsqrt(v + 1e-8) + 0.1 * w
    return (w - 0.02 * step).astype(jnp.bfloat16), m, v


def clipped(gradients, sum_of_squares, count):
    factor = jnp.minimum(1.0, 0.5 * lax.rsqrt(sum_of_squares / count + 1e-30))
    return [g * factor for g in gradients]


def reference(g_w_gate, g_w_up, g_w_down, w_gate, w_up, w_down, m_w_gate, m_w_up, m_w_down, v_w_gate, v_w_up, v_w_down):
    def total(terms):
        return lax.scan(lambda so_far, term: (so_far + term.astype(jnp.float32), None), jnp.zeros(terms.shape[1:], jnp.float32), terms)[0]

    gradients = [total(terms).astype(jnp.bfloat16).astype(jnp.float32) for terms in (g_w_gate, g_w_up, g_w_down)]
    gradients = clipped(gradients, sum(jnp.sum(g * g) for g in gradients), sum(g.size for g in gradients))
    new = [
        adamw(w.astype(jnp.float32), m, v, g)
        for w, m, v, g in zip((w_gate, w_up, w_down), (m_w_gate, m_w_up, m_w_down), (v_w_gate, v_w_up, v_w_down), gradients, strict=True)
    ]
    return tuple(one[which] for which in range(3) for one in new)
```

```python
import jax
import jax.numpy as jnp
from jax import lax
from jax.experimental import pallas as pl
from jax.experimental.pallas import tpu as pltpu
from jax.sharding import PartitionSpec as P

MESH = pl.DeviceIdType.MESH
F32, BF16 = jnp.float32, jnp.bfloat16
ANY = pl.BlockSpec(memory_space=pl.ANY)


class Place:
    def __init__(self):
        self.rep, d = lax.axis_index("rep"), lax.axis_index("dp")
        self.x, self.y, self.z, self.c = d // 16, lax.rem(d // 8, 2), lax.rem(d // 2, 4), lax.rem(d, 2)
        low = self.z < 2
        self.low = low
        self.mz = jnp.where(low, self.z, 3 - self.z)
        self.end, self.inner = self.mz == 0, self.mz == 1
        self.far = self.dev(self.x, self.y, jnp.where(low, self.z + 1, self.z - 1), self.c)
        self.near = self.dev(self.x, self.y, jnp.where(low, 0, 3), self.c)
        self.nx = self.dev(1 - self.x, self.y, self.z, self.c)
        self.ny = self.dev(self.x, 1 - self.y, self.z, self.c)
        self.nc = self.dev(self.x, self.y, self.z, 1 - self.c)
        self.qo = self.x * 2 + self.y
        self.qx = (1 - self.x) * 2 + self.y
        self.qy = self.x * 2 + 1 - self.y
        self.qd = (1 - self.x) * 2 + 1 - self.y

    def dev(self, x, y, z, c):
        return (self.rep, ((x * 2 + y) * 4 + z) * 2 + c)

    def zi(self, m):
        return jnp.where(self.low, m, 3 - m)

    def line(self, k):
        return lax.rem(self.z + k, 4)

    def meet(self, peers):
        barrier = pltpu.get_barrier_semaphore()
        for p in peers:
            pl.semaphore_signal(barrier, inc=1, device_id=p, device_id_type=MESH)
        pl.semaphore_wait(barrier, len(peers))


def send(src, dst, s, r, to):
    pltpu.make_async_remote_copy(src_ref=src, dst_ref=dst, send_sem=s, recv_sem=r, device_id=to, device_id_type=MESH).start()


def arrived(ref, sem):
    pltpu.make_async_copy(ref, ref, sem).wait()


def add_into(dst, *srcs):
    rows, cols = dst.shape
    step = 16 if cols > 2048 else 32

    def strip(i, carry):
        at = pl.ds(pl.multiple_of(i * step, step), step)
        total = srcs[0][at, :].astype(F32)
        for s in srcs[1:]:
            total = total + s[at, :].astype(F32)
        dst[at, :] = total.astype(BF16)
        return carry

    lax.fori_loop(0, rows // step, strip, 0)


def each(n, body):
    lax.fori_loop(0, n, lambda i, carry: (body(i), carry)[1], 0)


TASKS = ["D0", "D1", "X0", "Y0", "D2", "X1", "Y1", "D3", "X2", "Y2", "O0", "D4", "X3", "Y3", "O1", "D5", "X4", "Y4", "O2", "X5", "Y5", "O3", "O4", "O5"]


def rs_kernel(*refs):
    terms, outs, theirs, total = refs[0:3], refs[3:6], refs[6:9], refs[9]
    wide, tall = refs[10:19], refs[19:28]
    sq, lz, lg, cs, cr, ls, xs, xr, ys, yr, zs, zr, osem, es, er = refs[28:]
    at = Place()
    group = (at.x * 2 + at.y) * 2 + at.c
    line_peers = [at.dev(at.x, at.y, at.line(k), at.c) for k in (1, 2, 3)]
    others = [lax.rem(group + k, 8) for k in range(1, 8)]
    group_peers = [at.dev(j // 4, lax.rem(j // 2, 2), at.z, lax.rem(j, 2)) for j in others]
    at.meet(line_peers + group_peers)
    columns = {"D": at.qd, "X": at.qx, "Y": at.qy, "O": at.qo}

    def parts(name):
        t = int(name[1])
        bufs = (wide, t) if t < 4 else (tall, t - 4)
        return t, terms[t // 2], theirs[t // 2], t % 2, columns[name[0]], bufs

    for k, name in enumerate(TASKS):
        t, g, p, layer, q, _ = parts(name)
        send(g.at[layer, q, :, 1 - at.c], p.at[layer, q], cs.at[k], cr.at[k], at.nc)

    slots, used = {}, {True: 0, False: 0}
    for name in TASKS:
        kind = int(name[1]) < 4
        slots[name] = used[kind] % 2
        used[kind] += 1

    def stage_of(name):
        t = int(name[1])
        return (wide if t < 4 else tall)[8].at[slots[name]], ls.at[0 if t < 4 else 1, slots[name]]

    def load(k):
        name = TASKS[k]
        t, g, p, layer, q, _ = parts(name)
        stage, sem = stage_of(name)
        pltpu.make_async_copy(g.at[layer, q, :, at.c], stage.at[0], sem.at[0]).start()
        arrived(p.at[layer, q], cr.at[k])
        pltpu.make_async_copy(p.at[layer, q], stage.at[1], sem.at[1]).start()

    sq[...] = jnp.zeros_like(sq)
    load(0)
    for k, name in enumerate(TASKS):
        if k + 1 < len(TASKS):
            load(k + 1)
        t, g, p, layer, q, (bufs, b) = parts(name)
        xf, yf, xin, yin, sd, rx, ry, zin = (r.at[b] for r in bufs[:8])
        stage, sem = stage_of(name)
        arrived(stage.at[0], sem.at[0])
        arrived(stage.at[1], sem.at[1])
        mine, yours = stage.at[0], stage.at[1]
        lower, upper = pl.ds(0, 2), pl.ds(2, 2)
        if name[0] == "D":
            each(4, lambda i: add_into(sd.at[i], mine.at[i], yours.at[i]))
            send(sd.at[lower], xf, xs.at[t, 0], xr.at[t, 0], at.nx)
            send(sd.at[upper], yf, ys.at[t, 0], yr.at[t, 0], at.ny)
        elif name[0] == "X":
            each(2, lambda i: add_into(rx.at[i], mine.at[i], yours.at[i]))
            send(rx, xin.at[lower], xs.at[t, 1], xr.at[t, 1], at.nx)
            arrived(yf, yr.at[t, 0])
            each(2, lambda i: add_into(yf.at[i], mine.at[i + 2], yours.at[i + 2], yf.at[i]))
            send(yf, xin.at[upper], xs.at[t, 2], xr.at[t, 2], at.nx)
        elif name[0] == "Y":
            each(2, lambda i: add_into(ry.at[i], mine.at[i + 2], yours.at[i + 2]))
            send(ry, yin.at[upper], ys.at[t, 1], yr.at[t, 1], at.ny)
            arrived(xf, xr.at[t, 0])
            each(2, lambda i: add_into(xf.at[i], mine.at[i], yours.at[i], xf.at[i]))
            send(xf, yin.at[lower], ys.at[t, 2], yr.at[t, 2], at.ny)
        else:
            arrived(xin.at[lower], xr.at[t, 1])
            arrived(yin.at[upper], yr.at[t, 1])
            arrived(yin.at[lower], yr.at[t, 2])
            arrived(xin.at[upper], xr.at[t, 2])

            def four(i):
                return mine.at[i], yours.at[i], xin.at[i], yin.at[i]

            @pl.when(at.end)
            def _():
                for m in (3, 2, 1):
                    i = at.zi(m)
                    add_into(xin.at[i], *four(i))
                    send(xin.at[i], zin.at[m - 1], zs.at[t, m - 1], zr.at[t, m - 1], at.far)

            @pl.when(at.inner)
            def _():
                for m in (3, 2):
                    i = at.zi(m)
                    arrived(zin.at[m - 1], zr.at[t, m - 1])
                    add_into(zin.at[m - 1], *four(i), zin.at[m - 1])
                    send(zin.at[m - 1], zin.at[6 - m], zs.at[t, m - 1], zr.at[t, 6 - m], at.far)
                i = at.zi(0)
                arrived(zin.at[3], zr.at[t, 3])
                add_into(zin.at[3], *four(i), zin.at[3])
                send(zin.at[3], zin.at[3], zs.at[t, 0], zr.at[t, 3], at.near)

            own = at.z

            @pl.when(at.end)
            def _():
                arrived(zin.at[3], zr.at[t, 3])
                add_into(yin.at[own], *four(own), zin.at[3])

            @pl.when(at.inner)
            def _():
                arrived(zin.at[0], zr.at[t, 0])
                arrived(zin.at[4], zr.at[t, 4])
                add_into(yin.at[own], *four(own), zin.at[0], zin.at[4])

            rows, cols = yin.shape[1:]
            step = 16 if cols > 2048 else 32

            def squares(i):
                g = yin[own, pl.ds(pl.multiple_of(i * step, step), step), :].astype(F32)
                g = g * g
                part = g[:, :128]
                for j in range(1, cols // 128):
                    part = part + g[:, j * 128 : j * 128 + 128]
                so_far = sq[...]
                for j in range(0, step, 8):
                    so_far = so_far + part[j : j + 8]
                sq[...] = so_far

            each(rows // step, squares)
            pltpu.make_async_copy(yin.at[own], outs[t // 2].at[layer], osem.at[t]).start()

    lz[at.z] = sq[...]
    for k in range(3):
        send(lz.at[at.z], lz.at[at.z], es.at[k], er.at[at.z], line_peers[k])
    for k in (1, 2, 3):
        arrived(lz.at[at.line(k)], er.at[at.line(k)])
    lg[group] = lz[0] + lz[1] + lz[2] + lz[3]
    for k in range(7):
        send(lg.at[group], lg.at[group], es.at[3 + k], er.at[4 + group], group_peers[k])
    for j in others:
        arrived(lg.at[j], er.at[4 + j])
    everything = lg[0]
    for j in range(1, 8):
        everything = everything + lg[j]
    total[...] = everything

    for k in range(3):
        arrived(lz.at[0], es.at[k])
    for k in range(7):
        arrived(lg.at[0], es.at[3 + k])
    for k, name in enumerate(TASKS):
        t, g, p, layer, q, _ = parts(name)
        arrived(p.at[layer, q], cs.at[k])
    for t in range(6):
        bufs, b = (wide, t) if t < 4 else (tall, t - 4)
        for j in range(3):
            arrived(bufs[0].at[b], xs.at[t, j])
            arrived(bufs[0].at[b], ys.at[t, j])
            arrived(bufs[7].at[b, 0], zs.at[t, j])
        arrived(outs[t // 2].at[t % 2], osem.at[t])


def summed(terms):
    DMA = pltpu.SemaphoreType.DMA

    def buffers(n, *block):
        return [pltpu.VMEM((n, k, *block), BF16) for k in (2, 2, 4, 4, 4, 2, 2, 5)] + [pltpu.VMEM((2, 2, 4, *block), BF16)]

    views = [t.reshape(2, 4, 4, 2, t.shape[1] // 32, t.shape[2]) for t in terms]
    blocks = [v.shape[4:] for v in views]
    result = pl.pallas_call(
        rs_kernel,
        out_shape=[jax.ShapeDtypeStruct((2, *b), BF16) for b in blocks]
        + [jax.ShapeDtypeStruct((2, 4, 4, *b), BF16) for b in blocks]
        + [jax.ShapeDtypeStruct((8, 128), F32)],
        in_specs=[ANY] * 3,
        out_specs=[ANY] * 6 + [pl.BlockSpec(memory_space=pltpu.VMEM)],
        scratch_shapes=buffers(4, *blocks[0])
        + buffers(2, *blocks[2])
        + [pltpu.VMEM((8, 128), F32), pltpu.VMEM((4, 8, 128), F32), pltpu.VMEM((8, 8, 128), F32)]
        + [DMA((24,)), DMA((24,)), DMA((2, 2, 2))]
        + [DMA((6, 3))] * 4
        + [DMA((6, 3)), DMA((6, 5)), DMA((6,)), DMA((10,)), DMA((12,))],
        compiler_params=pltpu.CompilerParams(collective_id=0, has_side_effects=True, vmem_limit_bytes=67043328),
        name="sum_terms",
    )(*views)
    return result[:3], jnp.sum(result[6])


def ag_kernel(*refs):
    new, outs = refs[0:3], refs[3:6]
    own, zs, zr, xs, xr, ys, yr, cs, cr = refs[6:]
    at = Place()
    at.meet([at.dev(at.x, at.y, at.line(k), at.c) for k in (1, 2, 3)] + [at.nx, at.ny, at.nc])
    three = range(3)

    def block(t, q, z):
        return outs[t].at[:, q, z, at.c]

    def zj(j):
        if j == 0:
            return at.z
        return at.zi(jnp.where(at.end, j, 0)) if j == 1 else at.zi(j)

    def spread(t, j, src, dst):
        send(src, dst, xs.at[t, j], xr.at[t, j], at.nx)
        send(src, dst, ys.at[t, j], yr.at[t, j], at.ny)
        send(src, dst, cs.at[t, 0, j], cr.at[t, 0, j], at.nc)

    for t in three:
        mine = block(t, at.qo, at.z)

        @pl.when(at.end)
        def _():
            send(new[t], mine, zs.at[t, 0], zr.at[t, 0], at.far)

        @pl.when(at.inner)
        def _():
            send(new[t], mine, zs.at[t, 0], zr.at[t, 1], at.far)
            send(new[t], mine, zs.at[t, 1], zr.at[t, 0], at.near)

        spread(t, 0, new[t], mine)
        pltpu.make_async_copy(new[t], mine, own.at[t]).start()
    for k in three:
        for t in three:
            piece = block(t, at.qo, zj(k + 1))
            arrived(piece, zr.at[t, k])

            @pl.when(at.inner)
            def _():
                if k == 0:
                    send(piece, piece, zs.at[t, 2], zr.at[t, 2], at.far)
                else:
                    send(piece, piece, zs.at[t, 2 + k], zr.at[t, k], at.near)

            spread(t, k + 1, piece, piece)
    for j in range(4):
        for t in three:
            piece = block(t, at.qx, zj(j))
            arrived(piece, xr.at[t, j])
            if j < 2:
                send(piece, piece, ys.at[t, 4 + j], yr.at[t, 4 + j], at.ny)
            send(piece, piece, cs.at[t, 1, j], cr.at[t, 1, j], at.nc)
            piece = block(t, at.qy, zj(j))
            arrived(piece, yr.at[t, j])
            if j >= 2:
                send(piece, piece, xs.at[t, 2 + j], xr.at[t, 2 + j], at.nx)
            send(piece, piece, cs.at[t, 2, j], cr.at[t, 2, j], at.nc)
    for j in range(4):
        for t in three:
            piece = block(t, at.qd, zj(j))
            arrived(piece, yr.at[t, 4 + j] if j < 2 else xr.at[t, 2 + j])
            send(piece, piece, cs.at[t, 3, j], cr.at[t, 3, j], at.nc)
    for t in three:
        piece = block(t, at.qo, at.z)
        for q in range(4):
            for j in range(4):
                arrived(piece, cr.at[t, q, j])
                arrived(piece, cs.at[t, q, j])
        for j in range(6):
            arrived(piece, xs.at[t, j])
            arrived(piece, ys.at[t, j])
        arrived(piece, own.at[t])
        arrived(piece, zs.at[t, 0])

        @pl.when(at.inner)
        def _():
            for j in range(1, 5):
                arrived(piece, zs.at[t, j])


def gathered(new):
    DMA = pltpu.SemaphoreType.DMA
    shapes = [(2, 4, 4, 2, *n.shape[1:]) for n in new]
    result = pl.pallas_call(
        ag_kernel,
        out_shape=[jax.ShapeDtypeStruct(s, BF16) for s in shapes],
        in_specs=[ANY] * 3,
        out_specs=[ANY] * 3,
        scratch_shapes=[DMA((3,)), DMA((3, 5)), DMA((3, 3))] + [DMA((3, 6))] * 4 + [DMA((3, 4, 4))] * 2,
        compiler_params=pltpu.CompilerParams(collective_id=1, has_side_effects=True),
        name="gather_weights",
    )(*new)
    return [r.reshape(2, 32 * n.shape[1], n.shape[2]) for r, n in zip(result, new, strict=True)]


def adamw(w, m, v, g):
    m = 0.9 * m + 0.1 * g
    v = 0.95 * v + 0.05 * g * g
    step = m * lax.rsqrt(v + 1e-8) + 0.1 * w
    return (w - 0.02 * step).astype(BF16), m, v


def solution(mesh):
    def step(*arrays):
        terms, weights, m, v = (arrays[i : i + 3] for i in (0, 3, 6, 9))
        gradients, squares = summed([t[0] for t in terms])
        count = 32 * sum(g.size for g in gradients)
        factor = jnp.minimum(1.0, 0.5 * lax.rsqrt(squares / count + 1e-30))
        me = lax.axis_index("dp")
        own = [lax.dynamic_slice_in_dim(w, me * one.shape[1], one.shape[1], 1).astype(F32) for w, one in zip(weights, m, strict=True)]
        new = [adamw(w, m, v, g.astype(F32) * factor) for w, m, v, g in zip(own, m, v, gradients, strict=True)]
        whole = gathered([one[0] for one in new])
        return (*whole, *(one[1] for one in new), *(one[2] for one in new))

    all_of, cut = P(None, None, None), P(None, "dp", None)
    return jax.shard_map(
        step,
        mesh=mesh,
        in_specs=(P(("rep", "dp"), None, None, None),) * 3 + (all_of,) * 3 + (cut,) * 6,
        out_specs=(P("rep", None, None),) * 3 + (P("rep", "dp", None),) * 6,
        check_vma=False,
    )
```

```python
import jax
import jax.numpy as jnp
from jax import lax
from jax.experimental import pallas as pl
from jax.experimental.pallas import tpu as pltpu
from jax.sharding import PartitionSpec as P

MESH = pl.DeviceIdType.MESH
F32, BF16 = jnp.float32, jnp.bfloat16
ANY = pl.BlockSpec(memory_space=pl.ANY)


class Place:
    def __init__(self):
        self.rep, d = lax.axis_index("rep"), lax.axis_index("dp")
        self.x, self.y, self.z, self.c = d // 16, lax.rem(d // 8, 2), lax.rem(d // 2, 4), lax.rem(d, 2)
        low = self.z < 2
        self.low = low
        self.mz = jnp.where(low, self.z, 3 - self.z)
        self.end, self.inner = self.mz == 0, self.mz == 1
        self.far = self.dev(self.x, self.y, jnp.where(low, self.z + 1, self.z - 1), self.c)
        self.near = self.dev(self.x, self.y, jnp.where(low, 0, 3), self.c)
        self.nx = self.dev(1 - self.x, self.y, self.z, self.c)
        self.ny = self.dev(self.x, 1 - self.y, self.z, self.c)
        self.nc = self.dev(self.x, self.y, self.z, 1 - self.c)
        self.qo = self.x * 2 + self.y
        self.qx = (1 - self.x) * 2 + self.y
        self.qy = self.x * 2 + 1 - self.y
        self.qd = (1 - self.x) * 2 + 1 - self.y

    def dev(self, x, y, z, c):
        return (self.rep, ((x * 2 + y) * 4 + z) * 2 + c)

    def zi(self, m):
        return jnp.where(self.low, m, 3 - m)

    def line(self, k):
        return lax.rem(self.z + k, 4)

    def meet(self, peers):
        barrier = pltpu.get_barrier_semaphore()
        for p in peers:
            pl.semaphore_signal(barrier, inc=1, device_id=p, device_id_type=MESH)
        pl.semaphore_wait(barrier, len(peers))


def send(src, dst, s, r, to):
    pltpu.make_async_remote_copy(src_ref=src, dst_ref=dst, send_sem=s, recv_sem=r, device_id=to, device_id_type=MESH).start()


def arrived(ref, sem):
    pltpu.make_async_copy(ref, ref, sem).wait()


def add_into(dst, *srcs):
    rows, cols = dst.shape
    step = 16 if cols > 2048 or rows % 32 else 32

    def strip(i, carry):
        at = pl.ds(pl.multiple_of(i * step, step), step)
        total = srcs[0][at, :].astype(F32)
        for s in srcs[1:]:
            total = total + s[at, :].astype(F32)
        dst[at, :] = total.astype(BF16)
        return carry

    lax.fori_loop(0, rows // step, strip, 0)


def each(n, body):
    lax.fori_loop(0, n, lambda i, carry: (body(i), carry)[1], 0)


TASKS = [
    "D4", "D0", "D1", "bS5Y", "D3", "bS5D", "D2", "Y0", "X0", "Y1", "bS5O", "Y2", "X1", "bF5D", "Y3", "bS5X", "X2", "bF5X", "X3", "bF5Y",
    "S0", "F0", "D6", "bH5D", "bH5Y", "S1", "bH5X", "S2", "H0", "F1", "X4", "H1", "F2", "S3", "bF5O", "Y4", "H2", "X6", "Y6", "E2", "bG5D",
    "bG5X", "F3", "bH5O", "E1", "H3", "E0", "S4", "F4", "S6", "bG5Y", "E3", "bK5X", "bK5Y", "H4", "F6", "E4", "H6", "bG5O", "E6",
]
WIDE, LATE = 4, 5


def meaning(name):
    if name[0] == "b":
        return name[:2], int(name[2]), name[3]
    return name[0], int(name[1]), name[0] if name[0] in "DXY" else "O"


def rs_kernel(*refs):
    terms, outs, theirs, total = refs[0:3], refs[3:6], refs[6:9], refs[9]
    wide, tall, late, stages = refs[10:18], refs[18:26], refs[26:34], refs[34:36]
    sq, lz, lg, cs, cr, ls, xs, xr, ys, yr, zs, zr, bzs, bzr, osem, es, er = refs[36:]
    at = Place()
    group = (at.x * 2 + at.y) * 2 + at.c
    line_peers = [at.dev(at.x, at.y, at.line(k), at.c) for k in (1, 2, 3)]
    others = [lax.rem(group + k, 8) for k in range(1, 8)]
    group_peers = [at.dev(j // 4, lax.rem(j // 2, 2), at.z, lax.rem(j, 2)) for j in others]
    at.meet(line_peers + group_peers)
    columns = {"D": at.qd, "X": at.qx, "Y": at.qy, "O": at.qo}
    tall_rows = tall[0].shape[2]

    def source(t):
        if t < WIDE:
            return t // 2, t % 2, pl.ds(0, wide[0].shape[2])
        if t == LATE:
            return 2, 1, pl.ds(0, 2 * tall_rows)
        return 2, 0, pl.ds((t - WIDE) // 2 * tall_rows, tall_rows)

    def half_of(name, c):
        _, t, col = meaning(name)
        weight, layer, rows = source(t)
        return terms[weight].at[layer, columns[col], :, c, rows], theirs[weight].at[layer, columns[col], :, rows]

    first = {}
    for name in TASKS:
        first.setdefault(meaning(name)[1:], name)
    order = list(first.values())
    for k, name in enumerate(order):
        g, p = half_of(name, 1 - at.c)
        send(g, p, cs.at[k], cr.at[k], at.nc)

    slots, used = {}, [0, 0]
    for name in TASKS:
        kind = int(meaning(name)[1] >= WIDE)
        slots[name] = (kind, used[kind] % 2)
        used[kind] += 1

    def staged(name):
        kind, slot = slots[name]
        t = meaning(name)[1]
        rows = pl.ds(0, source(t)[2].size)
        return [(stages[kind].at[slot, k, :, rows], ls.at[kind, slot, k]) for k in range(2)]

    def load(name):
        g, p = half_of(name, at.c)
        (mine, s), (yours, r) = staged(name)
        pltpu.make_async_copy(g, mine, s).start()
        if name in order:
            arrived(p, cr.at[order.index(name)])
        pltpu.make_async_copy(p, yours, r).start()

    def result(t):
        weight, layer, rows = source(t)
        return outs[weight].at[layer, rows]

    def finish(t, done):
        rows, cols = done.shape
        step = 16 if cols > 2048 or rows % 32 else 32

        def squares(i):
            g = done[pl.ds(pl.multiple_of(i * step, step), step), :].astype(F32)
            g = g * g
            part = g[:, :128]
            for j in range(1, cols // 128):
                part = part + g[:, j * 128 : j * 128 + 128]
            so_far = sq[...]
            for j in range(0, step, 8):
                so_far = so_far + part[j : j + 8]
            sq[...] = so_far

        each(rows // step, squares)
        pltpu.make_async_copy(done, result(t), osem.at[t]).start()


    def line_steps(step, zin, s, r, into, start):
        if step == "S":

            @pl.when(at.end)
            def _():
                for m in (3, 2, 1):
                    i = at.zi(m)
                    out = start(m, i)
                    into(out, i)
                    send(out, zin.at[m - 1], s.at[m - 1], r.at[m - 1], at.far)

        elif step == "F":

            @pl.when(at.inner)
            def _():
                for m in (3, 2):
                    arrived(zin.at[m - 1], r.at[m - 1])
                    into(zin.at[m - 1], at.zi(m), zin.at[m - 1])
                    send(zin.at[m - 1], zin.at[6 - m], s.at[m - 1], r.at[6 - m], at.far)

        elif step == "H":

            @pl.when(at.inner)
            def _():
                arrived(zin.at[3], r.at[3])
                into(zin.at[3], at.zi(0), zin.at[3])
                send(zin.at[3], zin.at[3], s.at[0], r.at[3], at.near)

        else:

            @pl.when(at.end)
            def _():
                arrived(zin.at[3], r.at[3])

            @pl.when(at.inner)
            def _():
                arrived(zin.at[0], r.at[0])
                arrived(zin.at[4], r.at[4])

    def plane_first(step, t, mine, yours):
        bufs, b = (wide, t) if t < WIDE else (tall, (t - WIDE) // 2)
        xf, yf, xin, yin, sd, rx, ry, zin = (r.at[b] for r in bufs)
        lower, upper = pl.ds(0, 2), pl.ds(2, 2)
        if step == "D":
            each(4, lambda i: add_into(sd.at[i], mine.at[i], yours.at[i]))
            send(sd.at[lower], xf, xs.at[t, 0], xr.at[t, 0], at.nx)
            send(sd.at[upper], yf, ys.at[t, 0], yr.at[t, 0], at.ny)
        elif step == "X":
            each(2, lambda i: add_into(rx.at[i], mine.at[i], yours.at[i]))
            send(rx, xin.at[lower], xs.at[t, 1], xr.at[t, 1], at.nx)
            arrived(yf, yr.at[t, 0])
            each(2, lambda i: add_into(yf.at[i], mine.at[i + 2], yours.at[i + 2], yf.at[i]))
            send(yf, xin.at[upper], xs.at[t, 2], xr.at[t, 2], at.nx)
        elif step == "Y":
            each(2, lambda i: add_into(ry.at[i], mine.at[i + 2], yours.at[i + 2]))
            send(ry, yin.at[upper], ys.at[t, 1], yr.at[t, 1], at.ny)
            arrived(xf, xr.at[t, 0])
            each(2, lambda i: add_into(xf.at[i], mine.at[i], yours.at[i], xf.at[i]))
            send(xf, yin.at[lower], ys.at[t, 2], yr.at[t, 2], at.ny)
        else:
            if step == "S":
                arrived(xin.at[lower], xr.at[t, 1])
                arrived(yin.at[upper], yr.at[t, 1])
                arrived(yin.at[lower], yr.at[t, 2])
                arrived(xin.at[upper], xr.at[t, 2])

            def into(dst, i, *more):
                add_into(dst, mine.at[i], yours.at[i], xin.at[i], yin.at[i], *more)

            line_steps(step, zin, zs.at[t], zr.at[t], into, lambda m, i: xin.at[i])
            if step == "E":
                own = yin.at[at.z]
                pl.when(at.end)(lambda: into(own, at.z, zin.at[3]))
                pl.when(at.inner)(lambda: into(own, at.z, zin.at[0], zin.at[4]))
                finish(t, own)

    def line_first(step, t, col, mine, yours):
        xf, yf, xin, yin, sd, rx, ry, zins = late
        n = "DXYO".index(col)
        zin = zins.at[n]
        lower, upper = pl.ds(0, tall_rows), pl.ds(tall_rows, tall_rows)

        def summed_z(dst, rows, *more):
            def into(*came):
                add_into(dst, mine.at[at.z, rows], yours.at[at.z, rows], *[zin.at[k, rows] for k in came], *more)

            pl.when(at.end)(lambda: into(3))
            pl.when(at.inner)(lambda: into(0, 4))

        def into(dst, i, *more):
            add_into(dst, mine.at[i], yours.at[i], *more)

        if step != "bK":
            line_steps(step[1], zin, bzs.at[n], bzr.at[n], into, lambda m, i: zin.at[m - 1])
        if step == "bG":
            if col == "D":
                summed_z(sd.at[lower], lower)
                summed_z(sd.at[upper], upper)
                send(sd.at[lower], xf, xs.at[t, 0], xr.at[t, 0], at.nx)
                send(sd.at[upper], yf, ys.at[t, 0], yr.at[t, 0], at.ny)
            elif col == "X":
                summed_z(rx, lower)
                send(rx, xin.at[lower], xs.at[t, 1], xr.at[t, 1], at.nx)
            elif col == "Y":
                summed_z(ry, upper)
                send(ry, yin.at[upper], ys.at[t, 1], yr.at[t, 1], at.ny)
            else:
                arrived(xin.at[lower], xr.at[t, 1])
                arrived(yin.at[upper], yr.at[t, 1])
                arrived(yin.at[lower], yr.at[t, 2])
                arrived(xin.at[upper], xr.at[t, 2])
                summed_z(yin.at[lower], lower, xin.at[lower], yin.at[lower])
                summed_z(yin.at[upper], upper, xin.at[upper], yin.at[upper])
                finish(t, yin)
        elif step == "bK" and col == "X":
            arrived(yf, yr.at[t, 0])
            summed_z(yf, upper, yf)
            send(yf, xin.at[upper], xs.at[t, 2], xr.at[t, 2], at.nx)
        elif step == "bK":
            arrived(xf, xr.at[t, 0])
            summed_z(xf, lower, xf)
            send(xf, yin.at[lower], ys.at[t, 2], yr.at[t, 2], at.ny)

    sq[...] = jnp.zeros_like(sq)
    load(TASKS[0])
    for k, name in enumerate(TASKS):
        if k + 1 < len(TASKS):
            load(TASKS[k + 1])
        step, t, col = meaning(name)
        (mine, s), (yours, r) = staged(name)
        arrived(mine, s)
        arrived(yours, r)
        if t == LATE:
            line_first(step, t, col, mine, yours)
        else:
            plane_first(step, t, mine, yours)

    lz[at.z] = sq[...]
    for k in range(3):
        send(lz.at[at.z], lz.at[at.z], es.at[k], er.at[at.z], line_peers[k])
    for k in (1, 2, 3):
        arrived(lz.at[at.line(k)], er.at[at.line(k)])
    lg[group] = lz[0] + lz[1] + lz[2] + lz[3]
    for k in range(7):
        send(lg.at[group], lg.at[group], es.at[3 + k], er.at[4 + group], group_peers[k])
    for j in others:
        arrived(lg.at[j], er.at[4 + j])
    everything = lg[0]
    for j in range(1, 8):
        everything = everything + lg[j]
    total[...] = everything

    for k in range(3):
        arrived(lz.at[0], es.at[k])
    for k in range(7):
        arrived(lg.at[0], es.at[3 + k])
    for k, name in enumerate(order):
        arrived(half_of(name, at.c)[1], cs.at[k])
    for t in range(7):
        bufs = wide if t < WIDE else tall
        for j in range(3):
            sent = late[0] if t == LATE else bufs[0].at[0]
            arrived(sent, xs.at[t, j])
            arrived(sent, ys.at[t, j])
            if t != LATE:
                arrived(bufs[7].at[0, 0], zs.at[t, j])
            else:
                for n in range(4):
                    arrived(late[7].at[0, 0], bzs.at[n, j])
        arrived(result(t), osem.at[t])


def summed(terms):
    DMA = pltpu.SemaphoreType.DMA

    def buffers(n, *block):
        return [pltpu.VMEM((n, k, *block), BF16) for k in (2, 2, 4, 4, 4, 2, 2, 5)]

    views = [t.reshape(2, 4, 4, 2, t.shape[1] // 32, t.shape[2]) for t in terms]
    blocks = [v.shape[4:] for v in views]
    low, (rows, cols) = blocks[0], blocks[2]
    late = [pltpu.VMEM((n, cols), BF16) for n in (rows // 2, rows // 2, rows, rows, rows, rows // 2, rows // 2)]
    result = pl.pallas_call(
        rs_kernel,
        out_shape=[jax.ShapeDtypeStruct((2, *b), BF16) for b in blocks]
        + [jax.ShapeDtypeStruct((2, 4, 4, *b), BF16) for b in blocks]
        + [jax.ShapeDtypeStruct((8, 128), F32)],
        in_specs=[ANY] * 3,
        out_specs=[ANY] * 6 + [pl.BlockSpec(memory_space=pltpu.VMEM)],
        scratch_shapes=buffers(WIDE, *low)
        + buffers(2, rows // 2, cols)
        + late
        + [pltpu.VMEM((4, 5, rows, cols), BF16)]
        + [pltpu.VMEM((2, 2, 4, *low), BF16), pltpu.VMEM((2, 2, 4, rows, cols), BF16)]
        + [pltpu.VMEM((8, 128), F32), pltpu.VMEM((4, 8, 128), F32), pltpu.VMEM((8, 8, 128), F32)]
        + [DMA((28,)), DMA((28,)), DMA((2, 2, 2))]
        + [DMA((7, 3))] * 4
        + [DMA((7, 3)), DMA((7, 5)), DMA((4, 3)), DMA((4, 5)), DMA((7,)), DMA((10,)), DMA((12,))],
        compiler_params=pltpu.CompilerParams(collective_id=0, has_side_effects=True, vmem_limit_bytes=67043328),
        name="sum_terms",
    )(*views)
    return result[:3], jnp.sum(result[6])


def ag_kernel(*refs):
    new, outs = refs[0:3], refs[3:6]
    own, zs, zr, bzs, bzr, xs, xr, ys, yr, cs, cr = refs[6:]
    at = Place()
    at.meet([at.dev(at.x, at.y, at.line(k), at.c) for k in (1, 2, 3)] + [at.nx, at.ny, at.nc])
    three = range(3)
    columns = (at.qo, at.qx, at.qy, at.qd)
    half = new[2].shape[1] // 2
    lower, upper = pl.ds(0, half), pl.ds(half, half)

    def mine(t):
        return new[t] if t < 2 else new[2].at[t - 2]

    def block(t, q, j):
        if j == 0:
            z = at.z
        else:
            z = at.zi(jnp.where(at.end, j, 0)) if j == 1 else at.zi(j)
        return outs[t].at[:, columns[q], z, at.c] if t < 2 else outs[2].at[t - 2, columns[q], z, at.c]

    def start_line(src, dst, s, r):
        @pl.when(at.end)
        def _():
            send(src, dst, s.at[0], r.at[0], at.far)

        @pl.when(at.inner)
        def _():
            send(src, dst, s.at[0], r.at[1], at.far)
            send(src, dst, s.at[1], r.at[0], at.near)

    def pass_line(k, piece, s, r):
        arrived(piece, r.at[k])

        @pl.when(at.inner)
        def _():
            if k == 0:
                send(piece, piece, s.at[2], r.at[2], at.far)
            else:
                send(piece, piece, s.at[2 + k], r.at[k], at.near)

    def to_core(t, q, j, src, dst):
        send(src, dst, cs.at[t, q, j], cr.at[t, q, j], at.nc)

    def spread(t, j, src, dst):
        send(src, dst, xs.at[t, j], xr.at[t, j], at.nx)
        send(src, dst, ys.at[t, j], yr.at[t, j], at.ny)
        to_core(t, 0, j, src, dst)

    def late_line(k):
        for q in range(4):
            piece = block(3, q, k + 1)
            pass_line(k, piece, bzs.at[q], bzr.at[q])
            to_core(3, q, k + 1, piece, piece)

    def diagonal(j):
        for t in three:
            piece = block(t, 1, j)
            arrived(piece, xr.at[t, j])
            if j < 2:
                send(piece, piece, ys.at[t, 4 + j], yr.at[t, 4 + j], at.ny)
            to_core(t, 1, j, piece, piece)
            piece = block(t, 2, j)
            arrived(piece, yr.at[t, j])
            if j >= 2:
                send(piece, piece, xs.at[t, 2 + j], xr.at[t, 2 + j], at.nx)
            to_core(t, 2, j, piece, piece)

    for t in three:
        start_line(mine(t), block(t, 0, 0), zs.at[t], zr.at[t])
        spread(t, 0, mine(t), block(t, 0, 0))
    spread(3, 0, mine(3), block(3, 0, 0))
    for t in range(4):
        pltpu.make_async_copy(mine(t), block(t, 0, 0), own.at[t]).start()
    for k in three:
        for t in three:
            piece = block(t, 0, k + 1)
            pass_line(k, piece, zs.at[t], zr.at[t])
            spread(t, k + 1, piece, piece)
        if k == 0:
            piece = block(3, 1, 0)
            arrived(piece, xr.at[3, 0])
            send(piece.at[lower], piece.at[lower], ys.at[3, 1], yr.at[3, 1], at.ny)
            to_core(3, 1, 0, piece, piece)
            piece = block(3, 2, 0)
            arrived(piece, yr.at[3, 0])
            send(piece.at[upper], piece.at[upper], xs.at[3, 1], xr.at[3, 1], at.nx)
            to_core(3, 2, 0, piece, piece)
        if k == 1:
            start_line(mine(3), block(3, 0, 0), bzs.at[0], bzr.at[0])
            for q in (1, 2):
                piece = block(3, q, 0)
                start_line(piece, piece, bzs.at[q], bzr.at[q])
    piece = block(3, 3, 0)
    arrived(piece.at[lower], yr.at[3, 1])
    arrived(piece.at[upper], xr.at[3, 1])
    start_line(piece, piece, bzs.at[3], bzr.at[3])
    to_core(3, 3, 0, piece, piece)
    diagonal(0)
    diagonal(1)
    late_line(0)
    diagonal(2)
    late_line(1)
    diagonal(3)
    late_line(2)
    for j in range(4):
        for t in three:
            piece = block(t, 3, j)
            arrived(piece, yr.at[t, 4 + j] if j < 2 else xr.at[t, 2 + j])
            to_core(t, 3, j, piece, piece)

    for t in range(4):
        piece = block(t, 0, 0)
        for q in range(4):
            for j in range(4):
                arrived(piece, cr.at[t, q, j])
                arrived(piece, cs.at[t, q, j])
        arrived(piece, own.at[t])
        for j in range(6 if t < 3 else 1):
            arrived(piece, xs.at[t, j])
            arrived(piece, ys.at[t, j])
        for s in [zs.at[t]] if t < 3 else [bzs.at[q] for q in range(4)]:
            arrived(piece, s.at[0])

            @pl.when(at.inner)
            def _():
                for j in range(1, 5):
                    arrived(piece, s.at[j])

    arrived(block(3, 0, 0).at[lower], xs.at[3, 1])
    arrived(block(3, 0, 0).at[lower], ys.at[3, 1])


def out_kernel(*refs):
    ins, outs, sems = refs[0:3], refs[3:6], refs[6]
    copies = [pltpu.make_async_copy(ins[t].at[layer], outs[t].at[layer], sems.at[t, layer]) for t in range(3) for layer in range(2)]
    for c in copies:
        c.start()
    for c in copies:
        c.wait()


def gathered(new):
    DMA = pltpu.SemaphoreType.DMA
    shapes = [(2, 4, 4, 2, *n.shape[1:]) for n in new]
    VMEM = pl.BlockSpec(memory_space=pltpu.VMEM)
    landed = pl.pallas_call(
        ag_kernel,
        out_shape=[pltpu.VMEM(s, BF16) for s in shapes],
        in_specs=[ANY] * 3,
        out_specs=[VMEM] * 3,
        scratch_shapes=[DMA((4,)), DMA((3, 5)), DMA((3, 3)), DMA((4, 5)), DMA((4, 3))] + [DMA((4, 6))] * 4 + [DMA((4, 4, 4))] * 2,
        compiler_params=pltpu.CompilerParams(collective_id=1, has_side_effects=True, vmem_limit_bytes=1 << 20),
        name="gather_weights",
    )(*new)
    result = pl.pallas_call(
        out_kernel,
        out_shape=[jax.ShapeDtypeStruct(s, BF16) for s in shapes],
        in_specs=[VMEM] * 3,
        out_specs=[ANY] * 3,
        scratch_shapes=[DMA((3, 2))],
        compiler_params=pltpu.CompilerParams(vmem_limit_bytes=1 << 20),
        name="write_weights",
    )(*[pltpu.with_memory_space_constraint(x, pltpu.VMEM) for x in landed])
    return [r.reshape(2, 32 * n.shape[1], n.shape[2]) for r, n in zip(result, new, strict=True)]


def adamw(w, m, v, g):
    m = 0.9 * m + 0.1 * g
    v = 0.95 * v + 0.05 * g * g
    step = m * lax.rsqrt(v + 1e-8) + 0.1 * w
    return (w - 0.02 * step).astype(BF16), m, v


def solution(mesh):
    def step(*arrays):
        terms, weights, m, v = (arrays[i : i + 3] for i in (0, 3, 6, 9))
        gradients, squares = summed([t[0] for t in terms])
        count = 32 * sum(g.size for g in gradients)
        factor = jnp.minimum(1.0, 0.5 * lax.rsqrt(squares / count + 1e-30))
        me = lax.axis_index("dp")
        own = [lax.dynamic_slice_in_dim(w, me * one.shape[1], one.shape[1], 1).astype(F32) for w, one in zip(weights, m, strict=True)]
        new = [adamw(w, m, v, g.astype(F32) * factor) for w, m, v, g in zip(own, m, v, gradients, strict=True)]
        whole = gathered([one[0] for one in new])
        return (*whole, *(one[1] for one in new), *(one[2] for one in new))

    all_of, cut = P(None, None, None), P(None, "dp", None)
    return jax.shard_map(
        step,
        mesh=mesh,
        in_specs=(P(("rep", "dp"), None, None, None),) * 3 + (all_of,) * 3 + (cut,) * 6,
        out_specs=(P("rep", None, None),) * 3 + (P("rep", "dp", None),) * 6,
        check_vma=False,
    )
```

```python
import jax
import jax.numpy as jnp
from jax import lax
from jax.experimental import pallas as pl
from jax.experimental.pallas import tpu as pltpu
from jax.sharding import PartitionSpec as P

MESH = pl.DeviceIdType.MESH
DMA = pltpu.SemaphoreType.DMA
F32, BF16 = jnp.float32, jnp.bfloat16
ANY = pl.BlockSpec(memory_space=pl.ANY)
VMEM = pl.BlockSpec(memory_space=pltpu.VMEM)


class Place:
    def __init__(self):
        self.rep, d = lax.axis_index("rep"), lax.axis_index("dp")
        self.x, self.y, self.z, self.c = d // 16, lax.rem(d // 8, 2), lax.rem(d // 2, 4), lax.rem(d, 2)
        low = self.z < 2
        self.low = low
        self.mz = jnp.where(low, self.z, 3 - self.z)
        self.end, self.inner = self.mz == 0, self.mz == 1
        self.far = self.dev(self.x, self.y, jnp.where(low, self.z + 1, self.z - 1), self.c)
        self.near = self.dev(self.x, self.y, jnp.where(low, 0, 3), self.c)
        self.nx = self.dev(1 - self.x, self.y, self.z, self.c)
        self.ny = self.dev(self.x, 1 - self.y, self.z, self.c)
        self.nc = self.dev(self.x, self.y, self.z, 1 - self.c)
        self.qo = self.x * 2 + self.y
        self.qx = (1 - self.x) * 2 + self.y
        self.qy = self.x * 2 + 1 - self.y
        self.qd = (1 - self.x) * 2 + 1 - self.y

    def dev(self, x, y, z, c):
        return (self.rep, ((x * 2 + y) * 4 + z) * 2 + c)

    def zi(self, m):
        return jnp.where(self.low, m, 3 - m)

    def line(self, k):
        return lax.rem(self.z + k, 4)

    def meet(self, peers):
        barrier = pltpu.get_barrier_semaphore()
        for p in peers:
            pl.semaphore_signal(barrier, inc=1, device_id=p, device_id_type=MESH)
        pl.semaphore_wait(barrier, len(peers))


def send(src, dst, s, r, to):
    pltpu.make_async_remote_copy(src_ref=src, dst_ref=dst, send_sem=s, recv_sem=r, device_id=to, device_id_type=MESH).start()


def arrived(ref, sem):
    pltpu.make_async_copy(ref, ref, sem).wait()


def halves(n):
    return pl.ds(0, n // 2), pl.ds(n // 2, n // 2)


def strips(shape, body):
    rows, cols = shape
    step = 16 if cols > 2048 or rows % 32 else 32

    def strip(i, carry):
        body(pl.ds(pl.multiple_of(i * step, step), step), step)
        return carry

    lax.fori_loop(0, rows // step, strip, 0)


def add_into(dst, *srcs):
    def strip(at, _):
        total = srcs[0][at, :].astype(F32)
        for s in srcs[1:]:
            total = total + s[at, :].astype(F32)
        dst[at, :] = total.astype(BF16)

    strips(dst.shape, strip)


def each(n, body):
    lax.fori_loop(0, n, lambda i, carry: (body(i), carry)[1], 0)


TYPES = [(0, 0, 0, 32), (0, 1, 0, 32), (1, 0, 0, 32), (1, 1, 0, 32), (2, 0, 0, 64), (2, 1, 0, 160), (2, 0, 64, 48), (2, 0, 112, 48)]
LATE = [5, 7]

TASKS = [
    "D4", "D0", "bS7D", "bS5D", "D1", "X0", "bS7O", "bS7Y", "Y0", "bS7X", "D2", "D3", "bF7Y", "bS5X", "Y1", "bF7D", "bS5O", "bF7X", "bH7D",
    "bF7O", "X1", "bF5X", "bF5D", "bH7Y", "Y2", "bS5Y", "X2", "X3", "bF5Y", "Y3", "S0", "D6", "bH5Y", "F0", "bH5D", "S1", "bH7X", "X4",
    "bF5O", "F1", "S2", "bG7D", "H1", "bG7Y", "H0", "F2", "bG5D", "bH5O", "bH5X", "H2", "S3", "E1", "bG7X", "X6", "Y4", "Y6", "F3", "H3",
    "bK7X", "bG5X", "S4", "bK5X", "E2", "bH7O", "bG5Y", "E0", "bK5Y", "F4", "S6", "E3", "bK7Y", "H4", "F6", "E4", "bG7O", "H6", "bG5O",
    "E6",
]


def meaning(name):
    if name[0] == "b":
        return name[:2], int(name[2]), name[3]
    return name[0], int(name[1]), name[0] if name[0] in "DXY" else "O"


def buffers(t, cols):
    rows = TYPES[t][3]
    if t in LATE:
        shapes = [(rows, cols // 2)] * 2 + [(rows, cols)] * 3 + [(rows, cols // 2)] * 2 + [(4, 5, rows, cols)]
    else:
        shapes = [(k, rows, cols) for k in (2, 2, 4, 4, 4, 2, 2, 5)]
    return [pltpu.VMEM(s, BF16) for s in shapes]


def rs_kernel(*refs):
    terms, outs, theirs, total, refs = refs[0:3], refs[3:6], refs[6:9], refs[9], list(refs[10:])
    bufs = [[refs.pop(0) for _ in range(8)] for _ in TYPES]
    stages = refs[:2]
    sq, lz, lg, cs, cr, ls, xs, xr, ys, yr, zs, zr, bzs, bzr, osem, es, er = refs[2:]
    at = Place()
    group = (at.x * 2 + at.y) * 2 + at.c
    line_peers = [at.dev(at.x, at.y, at.line(k), at.c) for k in (1, 2, 3)]
    others = [lax.rem(group + k, 8) for k in range(1, 8)]
    group_peers = [at.dev(j // 4, lax.rem(j // 2, 2), at.z, lax.rem(j, 2)) for j in others]
    at.meet(line_peers + group_peers)
    columns = {"D": at.qd, "X": at.qx, "Y": at.qy, "O": at.qo}

    def half_of(name, c):
        _, t, col = meaning(name)
        weight, layer, row, rows = TYPES[t]
        rows = pl.ds(row, rows)
        return terms[weight].at[layer, columns[col], :, c, rows], theirs[weight].at[layer, columns[col], :, rows]

    first = {}
    for name in TASKS:
        first.setdefault(meaning(name)[1:], name)
    order = list(first.values())
    for k, name in enumerate(order):
        g, p = half_of(name, 1 - at.c)
        send(g, p, cs.at[k], cr.at[k], at.nc)

    slots, used = {}, [0, 0]
    for name in TASKS:
        kind = TYPES[meaning(name)[1]][0] // 2
        slots[name] = (kind, used[kind] % 2)
        used[kind] += 1

    def staged(name):
        kind, slot = slots[name]
        rows = pl.ds(0, TYPES[meaning(name)[1]][3])
        return [(stages[kind].at[slot, k, :, rows], ls.at[kind, slot, k]) for k in range(2)]

    def load(name):
        g, p = half_of(name, at.c)
        (mine, s), (yours, r) = staged(name)
        pltpu.make_async_copy(g, mine, s).start()
        if name in order:
            arrived(p, cr.at[order.index(name)])
        pltpu.make_async_copy(p, yours, r).start()

    def result(t):
        weight, layer, row, rows = TYPES[t]
        return outs[weight].at[layer, pl.ds(row, rows)]

    def finish(t, done):
        def squares(rows, step):
            g = done[rows, :].astype(F32)
            g = g * g
            part = g[:, :128]
            for j in range(128, done.shape[1], 128):
                part = part + g[:, j : j + 128]
            so_far = sq[...]
            for j in range(0, step, 8):
                so_far = so_far + part[j : j + 8]
            sq[...] = so_far

        strips(done.shape, squares)
        pltpu.make_async_copy(done, result(t), osem.at[t]).start()

    def line_steps(step, zin, s, r, into, start):
        def pass_on(k, m, to, k_to, j):
            arrived(zin.at[k], r.at[k])
            into(zin.at[k], at.zi(m), zin.at[k])
            send(zin.at[k], zin.at[k_to], s.at[j], r.at[k_to], to)

        if step == "S":

            @pl.when(at.end)
            def _():
                for m in (3, 2, 1):
                    i = at.zi(m)
                    out = start(m - 1, i)
                    into(out, i)
                    send(out, zin.at[m - 1], s.at[m - 1], r.at[m - 1], at.far)

        elif step == "F":

            @pl.when(at.inner)
            def _():
                for m in (3, 2):
                    pass_on(m - 1, m, at.far, 6 - m, m - 1)

        elif step == "H":
            pl.when(at.inner)(lambda: pass_on(3, 0, at.near, 3, 0))
        else:

            @pl.when(at.end)
            def _():
                arrived(zin.at[3], r.at[3])

            @pl.when(at.inner)
            def _():
                for k in (0, 4):
                    arrived(zin.at[k], r.at[k])

    def run(step, t, col, mine, yours):
        xf, yf, xin, yin, sd, rx, ry, zin = bufs[t]
        late = t in LATE
        lower, upper = halves(xin.shape[0])
        if late:
            n = "DXYO".index(col)
            zin, s, r = zin.at[n], bzs.at[LATE.index(t), n], bzr.at[LATE.index(t), n]
            lower, upper = ((slice(None), cut) for cut in halves(xin.shape[1]))
            everything = (slice(None), slice(None))

            def plane(dst, cut, *more):
                def into(*came):
                    add_into(dst, mine.at[(at.z, *cut)], yours.at[(at.z, *cut)], *[zin.at[(k, *cut)] for k in came], *more)

                pl.when(at.end)(lambda: into(3))
                pl.when(at.inner)(lambda: into(0, 4))

            def into(dst, i, *more):
                add_into(dst, mine.at[i], yours.at[i], *more)
        else:
            s, r = zs.at[t], zr.at[t]
            everything = pl.ds(0, 4)

            def plane(dst, cut, *more):
                each(cut.size, lambda i: add_into(dst.at[i], *[ref.at[i + cut.start] for ref in (mine, yours)], *[ref.at[i] for ref in more]))

            def into(dst, i, *more):
                add_into(dst, mine.at[i], yours.at[i], xin.at[i], yin.at[i], *more)

        to_x = (xin, lower, upper, rx, yf, yr, xs, xr, at.nx)
        to_y = (yin, upper, lower, ry, xf, xr, ys, yr, at.ny)

        def arrivals():
            for dst, raw_cut, cut, _, _, _, _, there, _ in (to_x, to_y):
                arrived(dst.at[raw_cut], there.at[t, 1])
                arrived(dst.at[cut], there.at[t, 2])

        if late and step != "bK":
            line_steps(step[1], zin, s, r, into, lambda k, i: zin.at[k])
        elif not late and step in "SFHE":
            if step == "S":
                arrivals()
            line_steps(step, zin, s, r, into, lambda k, i: xin.at[i])
        if step in ("D", "bG") and col == "D":
            plane(sd, everything)
            send(sd.at[lower], xf, xs.at[t, 0], xr.at[t, 0], at.nx)
            send(sd.at[upper], yf, ys.at[t, 0], yr.at[t, 0], at.ny)
        elif col in "XY" and step in ("X", "Y", "bG", "bK"):
            dst, raw_cut, cut, raw, forward, came, sent, there, to = to_x if col == "X" else to_y
            if step != "bK":
                plane(raw, raw_cut)
                send(raw, dst.at[raw_cut], sent.at[t, 1], there.at[t, 1], to)
            if step != "bG":
                arrived(forward, came.at[t, 0])
                plane(forward, cut, forward)
                send(forward, dst.at[cut], sent.at[t, 2], there.at[t, 2], to)
        elif step == "bG":
            arrivals()
            plane(yin, everything, xin, yin)
            finish(t, yin)
        elif step == "E":
            own = yin.at[at.z]
            pl.when(at.end)(lambda: into(own, at.z, zin.at[3]))
            pl.when(at.inner)(lambda: into(own, at.z, zin.at[0], zin.at[4]))
            finish(t, own)

    sq[...] = jnp.zeros_like(sq)
    load(TASKS[0])
    for k, name in enumerate(TASKS):
        if k + 1 < len(TASKS):
            load(TASKS[k + 1])
        (mine, s), (yours, r) = staged(name)
        arrived(mine, s)
        arrived(yours, r)
        run(*meaning(name), mine, yours)

    lz[at.z] = sq[...]
    for k in range(3):
        send(lz.at[at.z], lz.at[at.z], es.at[k], er.at[at.z], line_peers[k])
    for k in (1, 2, 3):
        arrived(lz.at[at.line(k)], er.at[at.line(k)])
    lg[group] = lz[0] + lz[1] + lz[2] + lz[3]
    for k in range(7):
        send(lg.at[group], lg.at[group], es.at[3 + k], er.at[4 + group], group_peers[k])
    for j in others:
        arrived(lg.at[j], er.at[4 + j])
    everything = lg[0]
    for j in range(1, 8):
        everything = everything + lg[j]
    total[...] = everything

    for k in range(10):
        arrived(lz.at[0], es.at[k])
    for k, name in enumerate(order):
        arrived(half_of(name, at.c)[1], cs.at[k])
    for t in range(len(TYPES)):
        sent, line = bufs[t][0], bufs[t][7]
        for j in range(3):
            arrived(sent, xs.at[t, j])
            arrived(sent, ys.at[t, j])
            if t in LATE:
                for n in range(4):
                    arrived(line.at[0, 0], bzs.at[LATE.index(t), n, j])
            else:
                arrived(line.at[0], zs.at[t, j])
        arrived(result(t), osem.at[t])


def summed(terms):
    views = [t.reshape(2, 4, 4, 2, t.shape[1] // 32, t.shape[2]) for t in terms]
    blocks = [v.shape[4:] for v in views]
    types = len(TYPES)
    result = pl.pallas_call(
        rs_kernel,
        out_shape=[jax.ShapeDtypeStruct((2, *b), BF16) for b in blocks]
        + [jax.ShapeDtypeStruct((2, 4, 4, *b), BF16) for b in blocks]
        + [jax.ShapeDtypeStruct((8, 128), F32)],
        in_specs=[ANY] * 3,
        out_specs=[ANY] * 6 + [VMEM],
        scratch_shapes=[b for t in range(types) for b in buffers(t, blocks[TYPES[t][0]][1])]
        + [pltpu.VMEM((2, 2, 4, *blocks[k]), BF16) for k in (0, 2)]
        + [pltpu.VMEM((*n, 8, 128), F32) for n in ((), (4,), (8,))]
        + [DMA((4 * types,)), DMA((4 * types,)), DMA((2, 2, 2))]
        + [DMA((types, 3))] * 4
        + [DMA((types, 3)), DMA((types, 5)), DMA((2, 4, 3)), DMA((2, 4, 5)), DMA((types,)), DMA((10,)), DMA((12,))],
        compiler_params=pltpu.CompilerParams(collective_id=0, has_side_effects=True, vmem_limit_bytes=67043328),
        name="sum_terms",
    )(*views)
    return result[:3], result[6]


PARTS = [(0, None, 0, 32), (1, None, 0, 32), (2, 0, 0, 112), (2, 1, 0, 160), (2, 0, 112, 48)]

STEPS = [
    "o4", "o3", "o1", "p3", "o0", "o2", "l00", "l10", "s32", "s33", "p4", "l01", "l02", "s42", "s40", "l11", "y10", "l12", "l20", "x02",
    "x20", "s43", "y11", "l22", "b320", "s30", "y20", "s31", "y02", "b301", "l21", "y03", "x11", "b330", "b430", "b300", "b311", "y12",
    "x12", "y13", "b420", "y00", "b302", "s41", "x01", "f20", "b331", "b410", "b432", "x13", "f02", "b421", "y23", "b411", "x00", "b422",
    "x03", "b412", "b321", "y01", "x10", "b401", "b431", "f01", "f11", "b400", "f03", "y21", "x21", "b310", "x22", "y22", "x23", "b332",
    "b402", "b312", "b322", "f10", "f23", "f12", "f00", "f13", "f22", "f21",
]


def ag_kernel(*refs):
    new, outs = refs[0:3], refs[3:6]
    own, zs, zr, bzs, bzr, xs, xr, ys, yr, cs, cr = refs[6:]
    at = Place()
    at.meet([at.dev(at.x, at.y, at.line(k), at.c) for k in (1, 2, 3)] + [at.nx, at.ny, at.nc])
    columns = (at.qo, at.qx, at.qy, at.qd)
    lower, upper = halves(new[2].shape[2])

    def mine(t):
        weight, layer, row, rows = PARTS[t]
        return new[weight] if layer is None else new[weight].at[layer, pl.ds(row, rows)]

    def block(t, q, j):
        weight, layer, row, rows = PARTS[t]
        if j == 0:
            z = at.z
        else:
            z = at.zi(jnp.where(at.end, j, 0)) if j == 1 else at.zi(j)
        if layer is None:
            return outs[weight].at[:, columns[q], z, at.c]
        return outs[weight].at[layer, columns[q], z, at.c, pl.ds(row, rows)]

    def start_line(src, dst, s, r):
        @pl.when(at.end)
        def _():
            send(src, dst, s.at[0], r.at[0], at.far)

        @pl.when(at.inner)
        def _():
            send(src, dst, s.at[0], r.at[1], at.far)
            send(src, dst, s.at[1], r.at[0], at.near)

    def pass_line(k, piece, s, r):
        arrived(piece, r.at[k])

        @pl.when(at.inner)
        def _():
            if k == 0:
                send(piece, piece, s.at[2], r.at[2], at.far)
            else:
                send(piece, piece, s.at[2 + k], r.at[k], at.near)

    def to_core(t, q, j, src, dst):
        send(src, dst, cs.at[t, q, j], cr.at[t, q, j], at.nc)

    def spread(t, j, src, dst):
        send(src, dst, xs.at[t, j], xr.at[t, j], at.nx)
        send(src, dst, ys.at[t, j], yr.at[t, j], at.ny)
        to_core(t, 0, j, src, dst)

    def late(t):
        return bzs.at[t - 3], bzr.at[t - 3]

    def run(kind, t, *rest):
        if kind == "o":
            if t < 3:
                start_line(mine(t), block(t, 0, 0), zs.at[t], zr.at[t])
            spread(t, 0, mine(t), block(t, 0, 0))
        elif kind == "l":
            (k,) = rest
            piece = block(t, 0, k + 1)
            pass_line(k, piece, zs.at[t], zr.at[t])
            spread(t, k + 1, piece, piece)
        elif kind in "xy":
            (j,) = rest
            q, came = (1, xr) if kind == "x" else (2, yr)
            piece = block(t, q, j)
            arrived(piece, came.at[t, j])
            if kind == "x" and j < 2:
                send(piece, piece, ys.at[t, 4 + j], yr.at[t, 4 + j], at.ny)
            if kind == "y" and j >= 2:
                send(piece, piece, xs.at[t, 2 + j], xr.at[t, 2 + j], at.nx)
            to_core(t, q, j, piece, piece)
        elif kind == "f":
            (j,) = rest
            piece = block(t, 3, j)
            arrived(piece, yr.at[t, 4 + j] if j < 2 else xr.at[t, 2 + j])
            to_core(t, 3, j, piece, piece)
        elif kind == "p":
            for q, cut, came, s, r, to in ((1, lower, xr, ys, yr, at.ny), (2, upper, yr, xs, xr, at.nx)):
                piece = block(t, q, 0)
                arrived(piece, came.at[t, 0])
                send(piece.at[:, cut], piece.at[:, cut], s.at[t, 1], r.at[t, 1], to)
                to_core(t, q, 0, piece, piece)
        elif kind == "s":
            (q,) = rest
            piece = block(t, q, 0)
            if q == 3:
                arrived(piece.at[:, lower], yr.at[t, 1])
                arrived(piece.at[:, upper], xr.at[t, 1])
                to_core(t, q, 0, piece, piece)
            s, r = late(t)
            start_line(piece if q else mine(t), piece, s.at[q], r.at[q])
        else:
            q, k = rest
            piece = block(t, q, k + 1)
            s, r = late(t)
            pass_line(k, piece, s.at[q], r.at[q])
            to_core(t, q, k + 1, piece, piece)

    whole = [o.at[:, at.qo, at.z, at.c] for o in outs]
    started = False
    for step in STEPS:
        if step[0] != "o" and not started:
            started = True
            for w in range(3):
                pltpu.make_async_copy(new[w], whole[w], own.at[w]).start()
        run(step[0], *map(int, step[1:]))

    for t in range(len(PARTS)):
        piece = block(t, 0, 0)
        for q in range(4):
            for j in range(4):
                arrived(piece, cr.at[t, q, j])
                arrived(piece, cs.at[t, q, j])
        for j in range(6 if t < 3 else 1):
            arrived(piece, xs.at[t, j])
            arrived(piece, ys.at[t, j])
        if t >= 3:
            arrived(piece.at[:, lower], xs.at[t, 1])
            arrived(piece.at[:, lower], ys.at[t, 1])
        for s in [zs.at[t]] if t < 3 else [late(t)[0].at[q] for q in range(4)]:
            arrived(piece, s.at[0])

            @pl.when(at.inner)
            def _():
                for j in range(1, 5):
                    arrived(piece, s.at[j])

    for w in range(3):
        arrived(whole[w], own.at[w])


def out_kernel(*refs):
    ins, outs, sems = refs[0:3], refs[3:6], refs[6]
    copies = [pltpu.make_async_copy(ins[t].at[layer], outs[t].at[layer], sems.at[t, layer]) for t in range(3) for layer in range(2)]
    for c in copies:
        c.start()
    for c in copies:
        c.wait()


def gathered(new):
    shapes = [(2, 4, 4, 2, *n.shape[1:]) for n in new]
    landed = pl.pallas_call(
        ag_kernel,
        out_shape=[pltpu.VMEM(s, BF16) for s in shapes],
        in_specs=[ANY] * 3,
        out_specs=[VMEM] * 3,
        scratch_shapes=[DMA((3,)), DMA((3, 5)), DMA((3, 3)), DMA((2, 4, 5)), DMA((2, 4, 3))] + [DMA((5, 6))] * 4 + [DMA((5, 4, 4))] * 2,
        compiler_params=pltpu.CompilerParams(collective_id=1, has_side_effects=True, vmem_limit_bytes=1 << 20),
        name="gather_weights",
    )(*new)
    result = pl.pallas_call(
        out_kernel,
        out_shape=[jax.ShapeDtypeStruct(s, BF16) for s in shapes],
        in_specs=[VMEM] * 3,
        out_specs=[ANY] * 3,
        scratch_shapes=[DMA((3, 2))],
        compiler_params=pltpu.CompilerParams(vmem_limit_bytes=1 << 20),
        name="write_weights",
    )(*[pltpu.with_memory_space_constraint(x, pltpu.VMEM) for x in landed])
    return [r.reshape(2, 32 * n.shape[1], n.shape[2]) for r, n in zip(result, new, strict=True)]


def adamw_kernel(count, me, squares, *refs):
    g_in, w_in, m_in, v_in, w_out, m_out, v_out = (refs[i : i + 3] for i in range(0, 21, 3))
    factor = jnp.minimum(1.0, 0.5 * lax.rsqrt(jnp.sum(squares[...], keepdims=True) / count + 1e-30))
    for k in range(3):
        g = g_in[k][0].astype(F32) * factor
        m = 0.9 * m_in[k][0] + 0.1 * g
        v = 0.95 * v_in[k][0] + 0.05 * g * g
        w = w_in[k][0].astype(F32)
        w_out[k][0] = (w - 0.02 * (m * lax.rsqrt(v + 1e-8) + 0.1 * w)).astype(BF16)
        m_out[k][0] = m
        v_out[k][0] = v


def adamw(squares, g, w, m, v):
    cuts = 2
    count = 32 * sum(x.size for x in g)
    sizes = [(1, x.shape[1] // cuts, x.shape[2]) for x in g]
    own = [pl.BlockSpec(s, lambda layer, i, me: (layer, i, 0)) for s in sizes]
    of_all = [pl.BlockSpec(s, lambda layer, i, me: (layer, me[0] * cuts + i, 0)) for s in sizes]
    result = pl.pallas_call(
        lambda *refs: adamw_kernel(count, *refs),
        out_shape=[jax.ShapeDtypeStruct(x.shape, t) for t in (BF16, F32, F32) for x in g],
        grid_spec=pltpu.PrefetchScalarGridSpec(
            num_scalar_prefetch=1,
            grid=(2, cuts),
            in_specs=[pl.BlockSpec(squares.shape, lambda layer, i, me: (0, 0))] + own + of_all + own * 2,
            out_specs=own * 3,
        ),
        name="adamw",
    )(lax.axis_index("dp")[None], squares, *g, *w, *m, *v)
    return result[:3], result[3:6], result[6:]


def solution(mesh):
    def step(*arrays):
        terms, weights, m, v = (arrays[i : i + 3] for i in range(0, 12, 3))
        gradients, squares = summed([t[0] for t in terms])
        new, m, v = adamw(squares, gradients, weights, m, v)
        return (*gathered(new), *m, *v)

    all_of, cut = P(None, None, None), P(None, "dp", None)
    return jax.shard_map(
        step,
        mesh=mesh,
        in_specs=(P(("rep", "dp"), None, None, None),) * 3 + (all_of,) * 3 + (cut,) * 6,
        out_specs=(P("rep", None, None),) * 3 + (P("rep", "dp", None),) * 6,
        check_vma=False,
    )
```

```python
import functools

import jax
import jax.numpy as jnp
from jax import lax
from jax.experimental import pallas as pl
from jax.experimental.pallas import tpu as pltpu
from jax.sharding import PartitionSpec as P

MESH = pl.DeviceIdType.MESH
DMA = pltpu.SemaphoreType.DMA
F32, BF16 = jnp.float32, jnp.bfloat16
ANY = pl.BlockSpec(memory_space=pl.ANY)
VMEM = pl.BlockSpec(memory_space=pltpu.VMEM)


class Place:
    def __init__(self):
        self.rep, d = lax.axis_index("rep"), lax.axis_index("dp")
        self.x, self.y, self.z, self.c = d // 16, lax.rem(d // 8, 2), lax.rem(d // 2, 4), lax.rem(d, 2)
        low = self.z < 2
        self.low = low
        self.mz = jnp.where(low, self.z, 3 - self.z)
        self.end, self.inner = self.mz == 0, self.mz == 1
        self.far = self.dev(self.x, self.y, jnp.where(low, self.z + 1, self.z - 1), self.c)
        self.near = self.dev(self.x, self.y, jnp.where(low, 0, 3), self.c)
        self.nx = self.dev(1 - self.x, self.y, self.z, self.c)
        self.ny = self.dev(self.x, 1 - self.y, self.z, self.c)
        self.nc = self.dev(self.x, self.y, self.z, 1 - self.c)
        self.qo = self.x * 2 + self.y
        self.qx = (1 - self.x) * 2 + self.y
        self.qy = self.x * 2 + 1 - self.y
        self.qd = (1 - self.x) * 2 + 1 - self.y

    def dev(self, x, y, z, c):
        return (self.rep, ((x * 2 + y) * 4 + z) * 2 + c)

    def zi(self, m):
        return jnp.where(self.low, m, 3 - m)

    def line(self, k):
        return lax.rem(self.z + k, 4)

    def meet(self, peers):
        barrier = pltpu.get_barrier_semaphore()
        for p in peers:
            pl.semaphore_signal(barrier, inc=1, device_id=p, device_id_type=MESH)
        pl.semaphore_wait(barrier, len(peers))


def send(src, dst, s, r, to):
    pltpu.make_async_remote_copy(src_ref=src, dst_ref=dst, send_sem=s, recv_sem=r, device_id=to, device_id_type=MESH).start()


def arrived(ref, sem):
    pltpu.make_async_copy(ref, ref, sem).wait()


def halves(n):
    return pl.ds(0, n // 2), pl.ds(n // 2, n // 2)


def strips(shape, body):
    rows, cols = shape
    step = 16 if cols > 2048 or rows % 32 else 32

    def strip(i, carry):
        body(pl.ds(pl.multiple_of(i * step, step), step), step)
        return carry

    lax.fori_loop(0, rows // step, strip, 0)


def add_into(dst, *srcs):
    def strip(at, _):
        total = srcs[0][at, :].astype(F32)
        for s in srcs[1:]:
            total = total + s[at, :].astype(F32)
        dst[at, :] = total.astype(BF16)

    strips(dst.shape, strip)


def each(n, body):
    lax.fori_loop(0, n, lambda i, carry: (body(i), carry)[1], 0)


TYPES = [(0, 0, 0, 32), (0, 1, 0, 32), (1, 0, 0, 32), (1, 1, 0, 32), (2, 0, 0, 48), (2, 1, 0, 160), (2, 0, 48, 64), (2, 0, 112, 48)]
SLOTS = 3
LATE = [5, 7]

TASKS = [
    "D4", "bS7X", "D2", "bS5Y", "bS5X", "bS7Y", "D0", "D1", "bS7D", "X0", "Y0", "bF5Y", "Y1", "bF5X", "bS5O", "bH5Y", "bS5D", "bH5X", "D3",
    "Y2", "bF7Y", "X1", "S0", "bS7O", "bH7Y", "X2", "bF7X", "Y3", "bF5O", "bF7D", "bH7D", "X3", "D6", "bH7X", "S1", "F0", "bF5D", "F1",
    "S2", "bG7D", "bH5O", "H0", "X4", "bH5D", "H1", "F2", "S3", "bG7X", "Y4", "E1", "bF7O", "X6", "H2", "Y6", "bG5D", "F3", "bG5Y", "E0",
    "bH7O", "bK7X", "S4", "bG7Y", "bG5X", "H3", "E2", "F4", "S6", "bK7Y", "bK5X", "H4", "bK5Y", "F6", "bG7O", "E4", "H6", "E3", "bG5O",
    "E6",
]


def meaning(name):
    if name[0] == "b":
        return name[:2], int(name[2]), name[3]
    return name[0], int(name[1]), name[0] if name[0] in "DXY" else "O"


def buffers(t, cols):
    rows = TYPES[t][3]
    if t in LATE:
        shapes = [(rows, cols // 2)] * 2 + [(rows, cols)] * 3 + [(rows, cols // 2)] * 2 + [(4, 5, rows, cols)]
    else:
        shapes = [(k, rows, cols) for k in (2, 2, 4, 4, 4, 2, 2, 5)]
    return [pltpu.VMEM(s, BF16) for s in shapes]


def rs_kernel(*refs):
    terms, outs, theirs, total, refs = refs[0:3], refs[3:6], refs[6:9], refs[9], list(refs[10:])
    bufs = [[refs.pop(0) for _ in range(8)] for _ in TYPES]
    stages = refs[:2]
    sq, lz, lg, cs, cr, ls, xs, xr, ys, yr, zs, zr, bzs, bzr, osem, es, er = refs[2:]
    at = Place()
    group = (at.x * 2 + at.y) * 2 + at.c
    line_peers = [at.dev(at.x, at.y, at.line(k), at.c) for k in (1, 2, 3)]
    others = [lax.rem(group + k, 8) for k in range(1, 8)]
    group_peers = [at.dev(j // 4, lax.rem(j // 2, 2), at.z, lax.rem(j, 2)) for j in others]
    at.meet(line_peers + group_peers)
    columns = {"D": at.qd, "X": at.qx, "Y": at.qy, "O": at.qo}

    def half_of(name, c):
        _, t, col = meaning(name)
        weight, layer, row, rows = TYPES[t]
        rows = pl.ds(row, rows)
        return terms[weight].at[layer, columns[col], :, c, rows], theirs[weight].at[layer, columns[col], :, rows]

    first = {}
    for name in TASKS:
        first.setdefault(meaning(name)[1:], name)
    order = list(first.values())
    for k, name in enumerate(order):
        g, p = half_of(name, 1 - at.c)
        send(g, p, cs.at[k], cr.at[k], at.nc)

    slots, used = {}, [0, 0]
    for name in TASKS:
        kind = TYPES[meaning(name)[1]][0] // 2
        slots[name] = (kind, used[kind] % SLOTS)
        used[kind] += 1

    def staged(name):
        kind, slot = slots[name]
        rows = pl.ds(0, TYPES[meaning(name)[1]][3])
        return [(stages[kind].at[slot, k, :, rows], ls.at[kind, slot, k]) for k in range(2)]

    def where_used(name, body):
        step = meaning(name)[0][-1]
        if step in "SFH":
            pl.when(at.end if step == "S" else at.inner)(body)
        else:
            body()

    def load(name):
        g, p = half_of(name, at.c)
        (mine, s), (yours, r) = staged(name)
        if name in order:
            arrived(p, cr.at[order.index(name)])

        @functools.partial(where_used, name)
        def _():
            pltpu.make_async_copy(g, mine, s).start()
            pltpu.make_async_copy(p, yours, r).start()

    def result(t):
        weight, layer, row, rows = TYPES[t]
        return outs[weight].at[layer, pl.ds(row, rows)]

    def finish(t, done):
        def squares(rows, step):
            g = done[rows, :].astype(F32)
            g = g * g
            part = g[:, :128]
            for j in range(128, done.shape[1], 128):
                part = part + g[:, j : j + 128]
            so_far = sq[...]
            for j in range(0, step, 8):
                so_far = so_far + part[j : j + 8]
            sq[...] = so_far

        strips(done.shape, squares)
        pltpu.make_async_copy(done, result(t), osem.at[t]).start()

    def line_steps(step, zin, s, r, into, start):
        def pass_on(k, m, to, k_to, j):
            arrived(zin.at[k], r.at[k])
            into(zin.at[k], at.zi(m), zin.at[k])
            send(zin.at[k], zin.at[k_to], s.at[j], r.at[k_to], to)

        if step == "S":

            @pl.when(at.end)
            def _():
                for m in (3, 2, 1):
                    i = at.zi(m)
                    out = start(m - 1, i)
                    into(out, i)
                    send(out, zin.at[m - 1], s.at[m - 1], r.at[m - 1], at.far)

        elif step == "F":

            @pl.when(at.inner)
            def _():
                for m in (3, 2):
                    pass_on(m - 1, m, at.far, 6 - m, m - 1)

        elif step == "H":
            pl.when(at.inner)(lambda: pass_on(3, 0, at.near, 3, 0))
        else:

            @pl.when(at.end)
            def _():
                arrived(zin.at[3], r.at[3])

            @pl.when(at.inner)
            def _():
                for k in (0, 4):
                    arrived(zin.at[k], r.at[k])

    def run(step, t, col, mine, yours):
        xf, yf, xin, yin, sd, rx, ry, zin = bufs[t]
        late = t in LATE
        lower, upper = halves(xin.shape[0])
        if late:
            n = "DXYO".index(col)
            zin, s, r = zin.at[n], bzs.at[LATE.index(t), n], bzr.at[LATE.index(t), n]
            lower, upper = ((slice(None), cut) for cut in halves(xin.shape[1]))
            everything = (slice(None), slice(None))

            def plane(dst, cut, *more):
                def into(*came):
                    add_into(dst, mine.at[(at.z, *cut)], yours.at[(at.z, *cut)], *[zin.at[(k, *cut)] for k in came], *more)

                pl.when(at.end)(lambda: into(3))
                pl.when(at.inner)(lambda: into(0, 4))

            def into(dst, i, *more):
                add_into(dst, mine.at[i], yours.at[i], *more)
        else:
            s, r = zs.at[t], zr.at[t]
            everything = pl.ds(0, 4)

            def plane(dst, cut, *more):
                each(cut.size, lambda i: add_into(dst.at[i], *[ref.at[i + cut.start] for ref in (mine, yours)], *[ref.at[i] for ref in more]))

            def into(dst, i, *more):
                add_into(dst, mine.at[i], yours.at[i], xin.at[i], yin.at[i], *more)

        to_x = (xin, lower, upper, rx, yf, yr, xs, xr, at.nx)
        to_y = (yin, upper, lower, ry, xf, xr, ys, yr, at.ny)

        def arrivals():
            for dst, raw_cut, cut, _, _, _, _, there, _ in (to_x, to_y):
                arrived(dst.at[raw_cut], there.at[t, 1])
                arrived(dst.at[cut], there.at[t, 2])

        if late and step != "bK":
            line_steps(step[1], zin, s, r, into, lambda k, i: zin.at[k])
        elif not late and step in "SFHE":
            if step == "S":
                arrivals()
            line_steps(step, zin, s, r, into, lambda k, i: xin.at[i])
        if step in ("D", "bG") and col == "D":
            plane(sd, everything)
            send(sd.at[lower], xf, xs.at[t, 0], xr.at[t, 0], at.nx)
            send(sd.at[upper], yf, ys.at[t, 0], yr.at[t, 0], at.ny)
        elif col in "XY" and step in ("X", "Y", "bG", "bK"):
            dst, raw_cut, cut, raw, forward, came, sent, there, to = to_x if col == "X" else to_y
            if step != "bK":
                plane(raw, raw_cut)
                send(raw, dst.at[raw_cut], sent.at[t, 1], there.at[t, 1], to)
            if step != "bG":
                arrived(forward, came.at[t, 0])
                plane(forward, cut, forward)
                send(forward, dst.at[cut], sent.at[t, 2], there.at[t, 2], to)
        elif step == "bG":
            arrivals()
            plane(yin, everything, xin, yin)
            finish(t, yin)
        elif step == "E":
            own = yin.at[at.z]
            pl.when(at.end)(lambda: into(own, at.z, zin.at[3]))
            pl.when(at.inner)(lambda: into(own, at.z, zin.at[0], zin.at[4]))
            finish(t, own)

    sq[...] = jnp.zeros_like(sq)
    load(TASKS[0])
    loaded = 1
    for k, name in enumerate(TASKS):
        while loaded < min(len(TASKS), k + (SLOTS if k > len(order) else 2)):
            load(TASKS[loaded])
            loaded += 1
        (mine, s), (yours, r) = staged(name)

        @functools.partial(where_used, name)
        def _():
            arrived(mine, s)
            arrived(yours, r)

        run(*meaning(name), mine, yours)

    lz[at.z] = sq[...]
    for k in range(3):
        send(lz.at[at.z], lz.at[at.z], es.at[k], er.at[at.z], line_peers[k])
    for k in (1, 2, 3):
        arrived(lz.at[at.line(k)], er.at[at.line(k)])
    lg[group] = lz[0] + lz[1] + lz[2] + lz[3]
    for k in range(7):
        send(lg.at[group], lg.at[group], es.at[3 + k], er.at[4 + group], group_peers[k])
    for j in others:
        arrived(lg.at[j], er.at[4 + j])
    everything = lg[0]
    for j in range(1, 8):
        everything = everything + lg[j]
    total[...] = everything

    for k in range(10):
        arrived(lz.at[0], es.at[k])
    for k, name in enumerate(order):
        arrived(half_of(name, at.c)[1], cs.at[k])
    for t in range(len(TYPES)):
        sent, line = bufs[t][0], bufs[t][7]
        for j in range(3):
            arrived(sent, xs.at[t, j])
            arrived(sent, ys.at[t, j])
            if t in LATE:
                for n in range(4):
                    arrived(line.at[0, 0], bzs.at[LATE.index(t), n, j])
            else:
                arrived(line.at[0], zs.at[t, j])
        arrived(result(t), osem.at[t])


def summed(terms):
    views = [t.reshape(2, 4, 4, 2, t.shape[1] // 32, t.shape[2]) for t in terms]
    blocks = [v.shape[4:] for v in views]
    types = len(TYPES)
    result = pl.pallas_call(
        rs_kernel,
        out_shape=[jax.ShapeDtypeStruct((2, *b), BF16) for b in blocks]
        + [jax.ShapeDtypeStruct((2, 4, 4, *b), BF16) for b in blocks]
        + [jax.ShapeDtypeStruct((8, 128), F32)],
        in_specs=[ANY] * 3,
        out_specs=[ANY] * 6 + [VMEM],
        scratch_shapes=[b for t in range(types) for b in buffers(t, blocks[TYPES[t][0]][1])]
        + [pltpu.VMEM((SLOTS, 2, 4, *blocks[k]), BF16) for k in (0, 2)]
        + [pltpu.VMEM((*n, 8, 128), F32) for n in ((), (4,), (8,))]
        + [DMA((4 * types,)), DMA((4 * types,)), DMA((2, SLOTS, 2))]
        + [DMA((types, 3))] * 4
        + [DMA((types, 3)), DMA((types, 5)), DMA((2, 4, 3)), DMA((2, 4, 5)), DMA((types,)), DMA((10,)), DMA((12,))],
        compiler_params=pltpu.CompilerParams(collective_id=0, has_side_effects=True, vmem_limit_bytes=67043328),
        name="sum_terms",
    )(*views)
    return result[:3], result[6]


PARTS = [(0, None, 0, 32), (1, None, 0, 32), (2, 0, 0, 112), (2, 1, 0, 160), (2, 0, 112, 48)]

STEPS = [
    "o4", "o3", "o1", "p3", "o0", "o2", "l00", "l10", "s32", "s33", "p4", "l01", "l02", "s42", "s40", "l11", "y10", "l12", "l20", "x02",
    "x20", "s43", "y11", "l22", "b320", "s30", "y20", "s31", "y02", "b301", "l21", "y03", "x11", "b330", "b430", "b300", "b311", "y12",
    "x12", "y13", "b420", "y00", "b302", "s41", "x01", "f20", "b331", "b410", "b432", "x13", "f02", "b421", "y23", "b411", "x00", "b422",
    "x03", "b412", "b321", "y01", "x10", "b401", "b431", "f01", "f11", "b400", "f03", "y21", "x21", "b310", "x22", "y22", "x23", "b332",
    "b402", "b312", "b322", "f10", "f23", "f12", "f00", "f13", "f22", "f21",
]


def ag_kernel(*refs):
    new, outs = refs[0:3], refs[3:6]
    own, zs, zr, bzs, bzr, xs, xr, ys, yr, cs, cr = refs[6:]
    at = Place()
    at.meet([at.dev(at.x, at.y, at.line(k), at.c) for k in (1, 2, 3)] + [at.nx, at.ny, at.nc])
    columns = (at.qo, at.qx, at.qy, at.qd)
    lower, upper = halves(new[2].shape[2])

    def mine(t):
        weight, layer, row, rows = PARTS[t]
        return new[weight] if layer is None else new[weight].at[layer, pl.ds(row, rows)]

    def block(t, q, j):
        weight, layer, row, rows = PARTS[t]
        if j == 0:
            z = at.z
        else:
            z = at.zi(jnp.where(at.end, j, 0)) if j == 1 else at.zi(j)
        if layer is None:
            return outs[weight].at[:, columns[q], z, at.c]
        return outs[weight].at[layer, columns[q], z, at.c, pl.ds(row, rows)]

    def start_line(src, dst, s, r):
        @pl.when(at.end)
        def _():
            send(src, dst, s.at[0], r.at[0], at.far)

        @pl.when(at.inner)
        def _():
            send(src, dst, s.at[0], r.at[1], at.far)
            send(src, dst, s.at[1], r.at[0], at.near)

    def pass_line(k, piece, s, r):
        arrived(piece, r.at[k])

        @pl.when(at.inner)
        def _():
            if k == 0:
                send(piece, piece, s.at[2], r.at[2], at.far)
            else:
                send(piece, piece, s.at[2 + k], r.at[k], at.near)

    def to_core(t, q, j, src, dst):
        send(src, dst, cs.at[t, q, j], cr.at[t, q, j], at.nc)

    def spread(t, j, src, dst):
        send(src, dst, xs.at[t, j], xr.at[t, j], at.nx)
        send(src, dst, ys.at[t, j], yr.at[t, j], at.ny)
        to_core(t, 0, j, src, dst)

    def late(t):
        return bzs.at[t - 3], bzr.at[t - 3]

    def run(kind, t, *rest):
        if kind == "o":
            if t < 3:
                start_line(mine(t), block(t, 0, 0), zs.at[t], zr.at[t])
            spread(t, 0, mine(t), block(t, 0, 0))
        elif kind == "l":
            (k,) = rest
            piece = block(t, 0, k + 1)
            pass_line(k, piece, zs.at[t], zr.at[t])
            spread(t, k + 1, piece, piece)
        elif kind in "xy":
            (j,) = rest
            q, came = (1, xr) if kind == "x" else (2, yr)
            piece = block(t, q, j)
            arrived(piece, came.at[t, j])
            if kind == "x" and j < 2:
                send(piece, piece, ys.at[t, 4 + j], yr.at[t, 4 + j], at.ny)
            if kind == "y" and j >= 2:
                send(piece, piece, xs.at[t, 2 + j], xr.at[t, 2 + j], at.nx)
            to_core(t, q, j, piece, piece)
        elif kind == "f":
            (j,) = rest
            piece = block(t, 3, j)
            arrived(piece, yr.at[t, 4 + j] if j < 2 else xr.at[t, 2 + j])
            to_core(t, 3, j, piece, piece)
        elif kind == "p":
            for q, cut, came, s, r, to in ((1, lower, xr, ys, yr, at.ny), (2, upper, yr, xs, xr, at.nx)):
                piece = block(t, q, 0)
                arrived(piece, came.at[t, 0])
                send(piece.at[:, cut], piece.at[:, cut], s.at[t, 1], r.at[t, 1], to)
                to_core(t, q, 0, piece, piece)
        elif kind == "s":
            (q,) = rest
            piece = block(t, q, 0)
            if q == 3:
                arrived(piece.at[:, lower], yr.at[t, 1])
                arrived(piece.at[:, upper], xr.at[t, 1])
                to_core(t, q, 0, piece, piece)
            s, r = late(t)
            start_line(piece if q else mine(t), piece, s.at[q], r.at[q])
        else:
            q, k = rest
            piece = block(t, q, k + 1)
            s, r = late(t)
            pass_line(k, piece, s.at[q], r.at[q])
            to_core(t, q, k + 1, piece, piece)

    whole = [o.at[:, at.qo, at.z, at.c] for o in outs]
    started = False
    for step in STEPS:
        if step[0] != "o" and not started:
            started = True
            for w in range(3):
                pltpu.make_async_copy(new[w], whole[w], own.at[w]).start()
        run(step[0], *map(int, step[1:]))

    for t in range(len(PARTS)):
        piece = block(t, 0, 0)
        for q in range(4):
            for j in range(4):
                arrived(piece, cr.at[t, q, j])
                arrived(piece, cs.at[t, q, j])
        for j in range(6 if t < 3 else 1):
            arrived(piece, xs.at[t, j])
            arrived(piece, ys.at[t, j])
        if t >= 3:
            arrived(piece.at[:, lower], xs.at[t, 1])
            arrived(piece.at[:, lower], ys.at[t, 1])
        for s in [zs.at[t]] if t < 3 else [late(t)[0].at[q] for q in range(4)]:
            arrived(piece, s.at[0])

            @pl.when(at.inner)
            def _():
                for j in range(1, 5):
                    arrived(piece, s.at[j])

    for w in range(3):
        arrived(whole[w], own.at[w])


def out_kernel(*refs):
    ins, outs, sems = refs[0:3], refs[3:6], refs[6]
    copies = [pltpu.make_async_copy(ins[t].at[layer], outs[t].at[layer], sems.at[t, layer]) for t in range(3) for layer in range(2)]
    for c in copies:
        c.start()
    for c in copies:
        c.wait()


def gathered(new):
    shapes = [(2, 4, 4, 2, *n.shape[1:]) for n in new]
    landed = pl.pallas_call(
        ag_kernel,
        out_shape=[pltpu.VMEM(s, BF16) for s in shapes],
        in_specs=[ANY] * 3,
        out_specs=[VMEM] * 3,
        scratch_shapes=[DMA((3,)), DMA((3, 5)), DMA((3, 3)), DMA((2, 4, 5)), DMA((2, 4, 3))] + [DMA((5, 6))] * 4 + [DMA((5, 4, 4))] * 2,
        compiler_params=pltpu.CompilerParams(collective_id=1, has_side_effects=True, vmem_limit_bytes=1 << 20),
        name="gather_weights",
    )(*new)
    result = pl.pallas_call(
        out_kernel,
        out_shape=[jax.ShapeDtypeStruct(s, BF16) for s in shapes],
        in_specs=[VMEM] * 3,
        out_specs=[ANY] * 3,
        scratch_shapes=[DMA((3, 2))],
        compiler_params=pltpu.CompilerParams(vmem_limit_bytes=1 << 20),
        name="write_weights",
    )(*[pltpu.with_memory_space_constraint(x, pltpu.VMEM) for x in landed])
    return [r.reshape(2, 32 * n.shape[1], n.shape[2]) for r, n in zip(result, new, strict=True)]


def adamw_kernel(count, me, squares, *refs):
    g_in, w_in, m_in, v_in, w_out, m_out, v_out = (refs[i : i + 3] for i in range(0, 21, 3))
    factor = jnp.minimum(1.0, 0.5 * lax.rsqrt(jnp.sum(squares[...], keepdims=True) / count + 1e-30))
    for k in range(3):
        g = g_in[k][0].astype(F32) * factor
        m = 0.9 * m_in[k][0] + 0.1 * g
        v = 0.95 * v_in[k][0] + 0.05 * g * g
        w = w_in[k][0].astype(F32)
        w_out[k][0] = (w - 0.02 * (m * lax.rsqrt(v + 1e-8) + 0.1 * w)).astype(BF16)
        m_out[k][0] = m
        v_out[k][0] = v


def adamw(squares, g, w, m, v):
    cuts = 2
    count = 32 * sum(x.size for x in g)
    sizes = [(1, x.shape[1] // cuts, x.shape[2]) for x in g]
    own = [pl.BlockSpec(s, lambda layer, i, me: (layer, i, 0)) for s in sizes]
    of_all = [pl.BlockSpec(s, lambda layer, i, me: (layer, me[0] * cuts + i, 0)) for s in sizes]
    result = pl.pallas_call(
        lambda *refs: adamw_kernel(count, *refs),
        out_shape=[jax.ShapeDtypeStruct(x.shape, t) for t in (BF16, F32, F32) for x in g],
        grid_spec=pltpu.PrefetchScalarGridSpec(
            num_scalar_prefetch=1,
            grid=(2, cuts),
            in_specs=[pl.BlockSpec(squares.shape, lambda layer, i, me: (0, 0))] + own + of_all + own * 2,
            out_specs=own * 3,
        ),
        name="adamw",
    )(lax.axis_index("dp")[None], squares, *g, *w, *m, *v)
    return result[:3], result[3:6], result[6:]


def solution(mesh):
    def step(*arrays):
        terms, weights, m, v = (arrays[i : i + 3] for i in range(0, 12, 3))
        gradients, squares = summed([t[0] for t in terms])
        new, m, v = adamw(squares, gradients, weights, m, v)
        return (*gathered(new), *m, *v)

    all_of, cut = P(None, None, None), P(None, "dp", None)
    return jax.shard_map(
        step,
        mesh=mesh,
        in_specs=(P(("rep", "dp"), None, None, None),) * 3 + (all_of,) * 3 + (cut,) * 6,
        out_specs=(P("rep", None, None),) * 3 + (P("rep", "dp", None),) * 6,
        check_vma=False,
    )
```
